32 devices in a mesh: dp: 4 (over y, x), expert: 8 (over z, core).
Axes of the slice: x: 2, y: 2, z: 4, core: 2. Of those that a mesh axis runs over, the one named last changes fastest.
Arguments:
- out_grad: bfloat16 [512, 3072], P('expert', 'dp'), may hold values from -6 to 6
- gate_probs: bfloat16 [512, 2], P('expert'), may hold values from 0.049804688 to 1
- expert_ids: int32 [512, 2], P('expert'), may hold values from 0 to 3, all different within a row; in each aligned block of 64 rows (0 to 63, 64 to 127, ...) at most 40 rows name the same one
- saved_gate: bfloat16 [8, 320, 8192], P('expert', None, 'dp'), may hold values from -8 to 8
- saved_up: bfloat16 [8, 320, 8192], P('expert', None, 'dp'), may hold values from -6 to 6
- w_gate: bfloat16 [8, 3072, 8192], P('expert', None, 'dp'), may hold values from -0.109375 to 0.109375
- w_up: bfloat16 [8, 3072, 8192], P('expert', None, 'dp'), may hold values from -0.109375 to 0.109375
- w_down: bfloat16 [8, 8192, 3072], P('expert', 'dp'), may hold values from -0.046875 to 0.046875
Outputs:
- token_grads: bfloat16 [512, 3072], P('expert', 'dp')
The draws below stay inside these ranges and needn't reach their ends.
Inputs may be any that keep to these rules, and one draw needn't show every extreme that they name: `expert_ids`: the 2 ids of a row differ. Within the rows of one device (aligned blocks of 64 rows) no expert is named by more than 40 rows, a bound that some block reaches.
All inputs are finite; a program needn't handle non-finite values.
Results may differ from the reference program's by a relative error of at most 0.013.
Values may be sent and summed in bfloat16 or wider, within the bound.
A program may use at most 128 MiB of HBM per device.

```python
import math
import jax
import jax.numpy as jnp
import numpy as np
from jax import lax

D = 3072
FF = 16384
TOP = 2
SPLIT = 2
TOK_DEV = 64
EXPERTS = 4
TOKENS = 512
CAP = 40
SLOTS = 320
N_EXPERT = 8


def shard_levels(stream_key, shape, pieces, low, largest):
    level, own = 1.0, jax.random.fold_in(stream_key, 6)
    for dim, blocks in pieces:
        steps = jnp.exp(jax.random.uniform(jax.random.fold_in(own, dim), (blocks,), jnp.float32, low / len(pieces), largest / len(pieces)))
        level = level * jnp.repeat(steps, shape[dim] // blocks).reshape([-1 if axis == dim else 1 for axis in range(len(shape))])
    return level


def assign_block(stream_key, own, number, rows, number_of, top, most, slope):
    order = jax.random.permutation(stream_key, number_of)
    heavy_load, common = shares(number_of, rows * top, most, slope, True), shares(number_of, rows * top, most, slope, False)
    places = jnp.arange(number_of)

    def named(sizes, offset_by):
        used = int((sizes > 0).sum())
        fixed = max(1, used // 4)
        moved = fixed + (places - fixed + offset_by * (used - fixed)) % max(1, number_of - fixed)
        return jnp.zeros((number_of,), jnp.int32).at[order[jnp.where(places < fixed, places, moved)]].set(jnp.asarray(sizes, jnp.int32))

    sizes = jnp.where(number % 4 == 0, named(heavy_load, number // 4), named(common, number - number // 4 - 1))
    mixed = jax.random.permutation(jax.random.fold_in(own, 3), number_of)
    giver, sink = mixed[0:number_of // 2 * 2:2], mixed[1:number_of // 2 * 2:2]
    room = jnp.minimum(sizes[giver] - 1, most - sizes[sink]) // 2
    room = jnp.where((giver == order[0]) | (sink == order[0]) | (sizes[sink] == 0), 0, jnp.maximum(room, 0))
    moved = jax.random.randint(jax.random.fold_in(own, 4), (number_of // 2,), 0, 1 << 20) % (room + 1)
    sizes = sizes.at[giver].add(-moved).at[sink].add(moved)
    members = jnp.searchsorted(jnp.cumsum(sizes), jnp.arange(rows * top), side="right").astype(jnp.int32)
    grid = members.reshape(top, rows).T
    grid = grid[jax.random.permutation(jax.random.fold_in(own, 1), rows)]
    offset_by = jax.random.randint(jax.random.fold_in(own, 2), (rows, 1), 0, top)
    return jnp.take_along_axis(grid, (jnp.arange(top)[None, :] + offset_by) % top, axis=1)


def shares(number_of, total, most, skew, full):
    weights = [(1 << 20) // math.isqrt(standing ** skew) + 1 for standing in range(1, number_of + 1)]
    largest = most if full else min(most, max(-(-total // number_of), total * weights[0] // sum(weights)))
    least = 1 if total - largest >= number_of - 1 else 0
    counts, rest = [largest] + [least] * (number_of - 1), total - largest - least * (number_of - 1)
    while rest > 0:
        movable = [i for i in range(1, number_of) if counts[i] < largest] or [i for i in range(1, number_of) if counts[i] < most]
        pool, left = sum([weights[i] for i in movable]), rest
        for i in movable:
            addition = min(most - counts[i], max(1, left * weights[i] // pool), rest)
            counts[i] = counts[i] + addition
            rest = rest - addition
    return np.array(counts)


def centred(key, shape, scale, most, pieces=(), kind=jnp.bfloat16):
    entries = jax.random.normal(key, shape, jnp.float32) * scale
    if len(pieces) > 0:
        entries = shard_levels(key, shape, pieces, -0.22, 0.18) * entries
    return jnp.clip(entries, min=-most, max=most).astype(kind)


def setup_inputs(seed: int = 0) -> dict:
    seeds = jax.random.split(jax.random.key(seed), 9)
    out_grad = centred(seeds[0], (TOKENS, D), 1.0, 6.0, ((0, 8), (1, 4)))
    gate_probs = jnp.clip(jnp.exp(math.log(1.0) - 2.9996462 * jax.random.uniform(seeds[1], (TOKENS, TOP), jnp.float32) ** shard_levels(seeds[1], (TOKENS, TOP), ((0, 8),), -0.2, 0.2)), 0.049804688, 1.0).astype(jnp.bfloat16)
    expert_ids_keys = jax.random.split(jax.random.fold_in(seeds[2], 1), TOKENS // TOK_DEV)
    expert_ids_turns = jax.random.permutation(jax.random.fold_in(seeds[2], 3), TOKENS // TOK_DEV)
    expert_ids = jax.vmap(lambda own, number: assign_block(jax.random.fold_in(seeds[2], 2), own, number, TOK_DEV, EXPERTS, TOP, CAP, 1))(expert_ids_keys, expert_ids_turns).reshape((TOKENS, TOP))
    saved_gate = centred(seeds[3], (EXPERTS * SPLIT, SLOTS, FF // SPLIT), 1.5, 8.0, ((0, 8), (2, 4)))
    saved_up = centred(seeds[4], (EXPERTS * SPLIT, SLOTS, FF // SPLIT), 1.0, 6.0, ((0, 8), (2, 4)))
    w_gate = centred(seeds[5], (EXPERTS * SPLIT, D, FF // SPLIT), D ** -0.5, 0.109375, ((0, 8), (2, 4)))
    w_up = centred(seeds[6], (EXPERTS * SPLIT, D, FF // SPLIT), D ** -0.5, 0.109375, ((0, 8), (2, 4)))
    w_down = centred(seeds[7], (EXPERTS * SPLIT, FF // SPLIT, D), FF ** -0.5, 0.046875, ((0, 8), (1, 4)))
    return dict(out_grad=out_grad, gate_probs=gate_probs, expert_ids=expert_ids, saved_gate=saved_gate, saved_up=saved_up, w_gate=w_gate, w_up=w_up, w_down=w_down)


def slot_layout(expert_ids):
    experts_iota = jnp.arange(EXPERTS, dtype=jnp.int32)
    chosen = (expert_ids[:, :, None] == experts_iota[None, None, :]).astype(jnp.int32)
    per_token = jnp.sum(chosen, axis=1, dtype=jnp.int32)
    blocks = per_token.reshape(N_EXPERT, TOK_DEV, EXPERTS)
    ranked = (jnp.cumsum(blocks, axis=1, dtype=jnp.int32) - blocks).reshape(TOKENS, EXPERTS)
    position = jnp.sum(chosen * ranked[:, None, :], axis=2, dtype=jnp.int32)
    source = jnp.arange(TOKENS, dtype=jnp.int32) // TOK_DEV
    return (source[:, None] * CAP + position).astype(jnp.int32)


def join_parts(array):
    parts, rows, width = array.shape
    split = array.reshape(EXPERTS, SPLIT, rows, width)
    return split.transpose(0, 2, 1, 3).reshape(EXPERTS, rows, SPLIT * width)


def expert_backward(inputs):
    slot_grad, slot_prob, gate_pre, up_pre, gate_weight, up_weight, down_weight = inputs
    projected = jnp.dot(slot_grad, down_weight.T, preferred_element_type=jnp.float32)
    gate_pre = gate_pre.astype(jnp.float32)
    up_pre = up_pre.astype(jnp.float32)
    sigmoid_gate = jax.nn.sigmoid(gate_pre)
    hidden_grad = slot_prob.astype(jnp.float32)[:, None] * projected
    gate_grad = (hidden_grad * up_pre * sigmoid_gate * (1.0 + gate_pre * (1.0 - sigmoid_gate))).astype(jnp.bfloat16)
    up_grad = (hidden_grad * gate_pre * sigmoid_gate).astype(jnp.bfloat16)
    summed = jnp.dot(gate_grad, gate_weight.T, preferred_element_type=jnp.float32)
    summed = summed + jnp.dot(up_grad, up_weight.T, preferred_element_type=jnp.float32)
    return summed.astype(jnp.bfloat16)


def reference(out_grad, gate_probs, expert_ids, saved_gate, saved_up, w_gate, w_up, w_down):
    slot_ids = slot_layout(expert_ids)
    spread = jnp.broadcast_to(out_grad[:, None, :], (TOKENS, TOP, D))
    slot_grads = jnp.zeros((EXPERTS, SLOTS, D), jnp.bfloat16).at[expert_ids, slot_ids].set(spread)
    slot_probs = jnp.zeros((EXPERTS, SLOTS), jnp.bfloat16).at[expert_ids, slot_ids].set(gate_probs)
    gate_full = join_parts(saved_gate)
    up_full = join_parts(saved_up)
    gate_weights = join_parts(w_gate)
    up_weights = join_parts(w_up)
    down_weights = w_down.reshape(EXPERTS, FF, D)
    slot_back = lax.map(expert_backward, (slot_grads, slot_probs, gate_full, up_full, gate_weights, up_weights, down_weights))
    picked = slot_back[expert_ids, slot_ids].astype(jnp.float32)
    return jnp.sum(picked, axis=1).astype(jnp.bfloat16)
```

```python
import functools

import jax
import jax.numpy as jnp
from jax import lax
from jax.experimental import pallas as pl
from jax.experimental.pallas import tpu as pltpu
from jax.sharding import PartitionSpec as P

SPLIT = 2
MESH = pl.DeviceIdType.MESH
TILE = 256
NT = (((1,), (1,)), ((), ()))
RETURN_ORDER = (3, 1, 2, 0)


def layer_kernel(
    experts, capacity, columns, hidden,
    ids_ref, ids_t_ref, probs_t_ref, grad_ref, gate_hbm, up_hbm, wg_hbm, wu_hbm, wd_hbm,
    out_ref,
    wd_v, wg_v, wu_v, gate_v, up_v, disp, zrecv, xbuf, xs, acc, gg, ug,
    pbuf, mine, pair_send, pair_recv, rs_send, rs_recv, back_send, back_recv,
    wd_sem, wg_sem, wu_sem, saved_sem,
    z_ss, z_rs, x_ss, x_rs, f_ss, f_rs, pair_ss, pair_rs, rs_ss, rs_rs, b_ss, b_rs,
):
    groups = experts * SPLIT
    tokens = grad_ref.shape[0]
    d = lax.axis_index("dp")
    g = lax.axis_index("expert")
    z, c = g // SPLIT, g % SPLIT
    sibling = z * SPLIT + (1 - c)
    dx, dy = d % 2, d // 2
    peers = (d, dy * 2 + (1 - dx), (1 - dy) * 2 + dx, (1 - dy) * 2 + (1 - dx))

    def block(r):
        return pl.ds(pl.multiple_of(peers[r] * columns, columns), columns)

    wd_copy = [pltpu.make_async_copy(wd_hbm.at[0, :, block(r)], wd_v.at[r], wd_sem.at[r]) for r in range(4)]
    wg_copy = [pltpu.make_async_copy(wg_hbm.at[0, block(r), :], wg_v.at[r], wg_sem.at[r]) for r in range(4)]
    wu_copy = [pltpu.make_async_copy(wu_hbm.at[0, block(r), :], wu_v.at[r], wu_sem.at[r]) for r in range(4)]
    gate_copy = pltpu.make_async_copy(gate_hbm.at[0], gate_v, saved_sem.at[0])
    up_copy = pltpu.make_async_copy(up_hbm.at[0], up_v, saved_sem.at[1])
    barrier = pltpu.get_barrier_semaphore()
    for k in range(1, experts):
        pl.semaphore_signal(
            barrier, inc=1, device_id=(d, ((z + k) % experts) * SPLIT + c), device_id_type=MESH
        )
    for r in range(1, 4):
        pl.semaphore_signal(barrier, inc=1, device_id=(peers[r], g), device_id_type=MESH)
    pl.semaphore_signal(barrier, inc=1, device_id=(d, sibling), device_id_type=MESH)
    for copy in wd_copy + [gate_copy, up_copy]:
        copy.start()
    for r in RETURN_ORDER:
        wg_copy[r].start()
        wu_copy[r].start()

    row = lax.broadcasted_iota(jnp.int32, (tokens, tokens), 0)
    col = lax.broadcasted_iota(jnp.int32, (tokens, tokens), 1)
    before = (row < col).astype(jnp.bfloat16)
    expert_row = lax.broadcasted_iota(jnp.int32, (8, tokens), 0)
    first, second = ids_t_ref[0:1, :] == expert_row, ids_t_ref[1:2, :] == expert_row
    named = jnp.where(first | second, 1.0, 0.0)
    weight = jnp.where(first, probs_t_ref[0:1, :], 0.0) + jnp.where(second, probs_t_ref[1:2, :], 0.0)
    rank = jnp.dot(named.astype(jnp.bfloat16), before, preferred_element_type=jnp.float32)
    place = lax.broadcasted_iota(jnp.int32, (capacity, tokens), 0).astype(jnp.float32)
    for e in range(experts):
        picked = jnp.where(place == rank[e : e + 1, :], weight[e : e + 1, :], 0.0)
        disp[e] = jnp.dot(
            picked.astype(jnp.bfloat16), grad_ref[...], preferred_element_type=jnp.float32
        ).astype(jnp.bfloat16)

    pl.semaphore_wait(barrier, experts + 3)

    def remote(src, dst, send, recv, device):
        return pltpu.make_async_remote_copy(
            src_ref=src, dst_ref=dst, send_sem=send, recv_sem=recv, device_id=device, device_id_type=MESH
        )

    def z_copies(src, dst, send, recv):
        copies = []
        for k in range(1, experts):
            to = (z + k) % experts
            copies.append(remote(src.at[to], dst.at[z], send.at[k], recv.at[k], (d, to * SPLIT + c)))
        return copies

    out_z = z_copies(disp, zrecv, z_ss, z_rs)
    for copy in out_z:
        copy.start()
    zrecv[z] = disp[z]
    for copy in out_z:
        copy.wait_recv()
    xbuf[0, c] = jnp.concatenate(
        [zrecv[s].astype(jnp.float32) for s in range(experts)], axis=0
    ).astype(jnp.bfloat16)
    out_x = [None] + [
        remote(xbuf.at[0, c], xbuf.at[r, c], x_ss.at[r], x_rs.at[r], (peers[r], g)) for r in range(1, 4)
    ]
    forward = [
        remote(xbuf.at[r, c], xbuf.at[r, c], f_ss.at[r], f_rs.at[r], (d, sibling)) for r in range(4)
    ]
    for r in (3, 1, 2):
        out_x[r].start()
    forward[0].start()

    def load_slots(r):
        halves = [xbuf[r, h].astype(jnp.float32) for h in range(SPLIT)]
        xs[...] = jnp.concatenate(
            [halves[i % SPLIT][(i // SPLIT) * capacity : (i // SPLIT + 1) * capacity] for i in range(groups)],
            axis=0,
        ).astype(jnp.bfloat16)

    for r in range(4):
        if r + 1 < 4:
            out_x[r + 1].wait_recv()
            forward[r + 1].start()
        forward[r].wait_recv()
        load_slots(r)
        wd_copy[r].wait()
        if r == 3:
            gate_copy.wait()
            up_copy.wait()

        def project(n, carry, r=r):
            here = pl.ds(pl.multiple_of(n * TILE, TILE), TILE)
            part = lax.dot_general(xs[...], wd_v[r, here, :], NT, preferred_element_type=jnp.float32)
            if r > 0:
                part = acc[:, here] + part
            if r < 3:
                acc[:, here] = part
            else:
                gate = gate_v[:, here].astype(jnp.float32)
                up = up_v[:, here].astype(jnp.float32)
                sig = jax.nn.sigmoid(gate)
                scaled = part * sig
                gg[:, here] = (scaled * up * (1.0 + gate * (1.0 - sig))).astype(jnp.bfloat16)
                ug[:, here] = (scaled * gate).astype(jnp.bfloat16)
            return carry

        lax.fori_loop(0, hidden // TILE, project, 0)

    pair = [
        remote(pair_send.at[r], pair_recv.at[r], pair_ss.at[r], pair_rs.at[r], (d, sibling)) for r in range(4)
    ]
    out_rs = [None] + [
        remote(rs_send.at[r], rs_recv.at[r], rs_ss.at[r], rs_rs.at[r], (peers[r], g)) for r in range(1, 4)
    ]

    def pass_on(r):
        pair[r].wait_recv()
        rs_send[r] = (mine[r] + pair_recv[r].astype(jnp.float32)).astype(jnp.bfloat16)
        out_rs[r].start()

    last = None
    for r in RETURN_ORDER:
        wg_copy[r].wait()
        wu_copy[r].wait()

        def back(n, carry, r=r):
            here = pl.ds(pl.multiple_of(n * TILE, TILE), TILE)
            part = lax.dot_general(gg[...], wg_v[r, here, :], NT, preferred_element_type=jnp.float32)
            part = part + lax.dot_general(ug[...], wu_v[r, here, :], NT, preferred_element_type=jnp.float32)
            for i in range(groups):
                pbuf[i, :, here] = part[i * capacity : (i + 1) * capacity]
            return carry

        lax.fori_loop(0, columns // TILE, back, 0)
        pair_send[r] = jnp.concatenate(
            [pbuf[s * SPLIT + (1 - c)] for s in range(experts)], axis=0
        ).astype(jnp.bfloat16)
        pair[r].start()
        mine[r] = jnp.concatenate([pbuf[s * SPLIT + c] for s in range(experts)], axis=0)
        if last is not None:
            pass_on(last)
        last = r

    pair[0].wait_recv()
    total = mine[0] + pair_recv[0].astype(jnp.float32)
    for r in (1, 2, 3):
        out_rs[r].wait_recv()
        total = total + rs_recv[r].astype(jnp.float32)
    for s in range(experts):
        back_send[s] = total[s * capacity : (s + 1) * capacity].astype(jnp.bfloat16)
    out_b = z_copies(back_send, back_recv, b_ss, b_rs)
    for copy in out_b:
        copy.start()
    back_recv[z] = back_send[z]

    after = (col < row).astype(jnp.bfloat16)
    expert_col = lax.broadcasted_iota(jnp.int32, (tokens, 128), 1)
    named_t = (ids_ref[:, 0:1] == expert_col) | (ids_ref[:, 1:2] == expert_col)
    named_t = jnp.where(named_t, 1.0, 0.0)
    rank_t = jnp.dot(after, named_t.astype(jnp.bfloat16), preferred_element_type=jnp.float32)
    place_t = lax.broadcasted_iota(jnp.int32, (tokens, capacity), 1).astype(jnp.float32)
    pickers = [
        jnp.where(place_t == rank_t[:, e : e + 1], named_t[:, e : e + 1], 0.0).astype(jnp.bfloat16)
        for e in range(experts)
    ]
    for copy in out_b:
        copy.wait_recv()
    result = jnp.dot(pickers[0], back_recv[0], preferred_element_type=jnp.float32)
    for e in range(1, experts):
        result = result + jnp.dot(pickers[e], back_recv[e], preferred_element_type=jnp.float32)
    out_ref[...] = result.astype(jnp.bfloat16)
    for copy in out_z + out_x[1:] + forward + pair + out_rs[1:] + out_b:
        copy.wait_send()


def local(out_grad, gate_probs, expert_ids, saved_gate, saved_up, w_gate, w_up, w_down):
    groups = lax.axis_size("expert")
    experts = groups // SPLIT
    tokens, columns = out_grad.shape
    slots, hidden = saved_gate.shape[1:]
    capacity = slots // groups
    half = experts * capacity
    vmem = pl.BlockSpec(memory_space=pltpu.VMEM)
    hbm = pl.BlockSpec(memory_space=pl.ANY)
    bf16, f32 = jnp.bfloat16, jnp.float32
    dma = pltpu.SemaphoreType.DMA
    return pl.pallas_call(
        functools.partial(layer_kernel, experts, capacity, columns, hidden),
        out_shape=jax.ShapeDtypeStruct((tokens, columns), bf16),
        in_specs=[vmem] * 4 + [hbm] * 5,
        out_specs=vmem,
        scratch_shapes=[
            pltpu.VMEM((4, hidden, columns), bf16),
            pltpu.VMEM((4, columns, hidden), bf16),
            pltpu.VMEM((4, columns, hidden), bf16),
            pltpu.VMEM((slots, hidden), bf16),
            pltpu.VMEM((slots, hidden), bf16),
            pltpu.VMEM((experts, capacity, columns), bf16),
            pltpu.VMEM((experts, capacity, columns), bf16),
            pltpu.VMEM((4, SPLIT, half, columns), bf16),
            pltpu.VMEM((slots, columns), bf16),
            pltpu.VMEM((slots, hidden), f32),
            pltpu.VMEM((slots, hidden), bf16),
            pltpu.VMEM((slots, hidden), bf16),
            pltpu.VMEM((groups, capacity, columns), f32),
            pltpu.VMEM((4, half, columns), f32),
            pltpu.VMEM((4, half, columns), bf16),
            pltpu.VMEM((4, half, columns), bf16),
            pltpu.VMEM((4, half, columns), bf16),
            pltpu.VMEM((4, half, columns), bf16),
            pltpu.VMEM((experts, capacity, columns), bf16),
            pltpu.VMEM((experts, capacity, columns), bf16),
            dma((4,)), dma((4,)), dma((4,)), dma((2,)),
            dma((experts,)), dma((experts,)),
            dma((4,)), dma((4,)), dma((4,)), dma((4,)), dma((4,)), dma((4,)), dma((4,)), dma((4,)),
            dma((experts,)), dma((experts,)),
        ],
        compiler_params=pltpu.CompilerParams(
            collective_id=0, has_side_effects=True, vmem_limit_bytes=67043328
        ),
    )(
        expert_ids, expert_ids.T, gate_probs.T.astype(f32), out_grad,
        saved_gate, saved_up, w_gate, w_up, w_down,
    )


def plain_local(out_grad, gate_probs, expert_ids, saved_gate, saved_up, w_gate, w_up, w_down):
    groups = lax.axis_size("expert")
    experts = groups // SPLIT
    columns = out_grad.shape[1]
    tok_rows = out_grad.shape[0]
    slot_count = saved_gate.shape[1]
    capacity = slot_count // groups
    experts_iota = jnp.arange(experts, dtype=jnp.int32)
    chosen = (expert_ids[:, :, None] == experts_iota[None, None, :]).astype(jnp.int32)
    per_token = jnp.sum(chosen, axis=1, dtype=jnp.int32)
    ranked = jnp.cumsum(per_token, axis=0, dtype=jnp.int32) - per_token
    position = jnp.sum(chosen * ranked[:, None, :], axis=2, dtype=jnp.int32)
    target = expert_ids * capacity + position
    slot_iota = jnp.arange(experts * capacity, dtype=jnp.int32)
    matches = slot_iota[:, None, None] == target[None, :, :]
    picker = jnp.any(matches, axis=2).astype(jnp.bfloat16)
    picker = jnp.repeat(picker.reshape(experts, capacity, tok_rows), SPLIT, axis=0).reshape(
        groups * capacity, tok_rows
    )
    weighted = jnp.where(matches, gate_probs.astype(jnp.float32)[None, :, :], 0.0)
    prob_slots = jnp.sum(weighted, axis=(1, 2)).astype(jnp.bfloat16).reshape(experts, capacity)
    prob_slots = jnp.repeat(prob_slots, SPLIT, axis=0)
    down_here = w_down[0]
    dispatched = jnp.dot(picker, out_grad, preferred_element_type=jnp.float32).astype(jnp.bfloat16)
    arrived, arrived_probs = (
        lax.all_to_all(
            dispatched.reshape(groups, capacity, columns),
            "expert",
            split_axis=0,
            concat_axis=0,
            tiled=True,
        ),
        lax.all_to_all(prob_slots, "expert", split_axis=0, concat_axis=0, tiled=True),
    )
    projected = lax.dot_general(
        lax.all_gather(arrived.reshape(slot_count, columns), "dp", axis=1, tiled=True),
        down_here,
        (((1,), (1,)), ((), ())),
        preferred_element_type=jnp.float32,
    )
    gate_pre = saved_gate[0].astype(jnp.float32)
    up_pre = saved_up[0].astype(jnp.float32)
    sigmoid_gate = jax.nn.sigmoid(gate_pre)
    hidden_grad = arrived_probs.reshape(slot_count).astype(jnp.float32)[:, None] * projected
    gate_grad = (
        hidden_grad * up_pre * sigmoid_gate * (1.0 + gate_pre * (1.0 - sigmoid_gate))
    ).astype(jnp.bfloat16)
    up_grad = (hidden_grad * gate_pre * sigmoid_gate).astype(jnp.bfloat16)
    gate_here = w_gate[0]
    up_here = w_up[0]
    first = lax.dot_general(
        gate_here, gate_grad, (((1,), (1,)), ((), ())), preferred_element_type=jnp.float32
    )
    second = lax.dot_general(
        up_here, up_grad, (((1,), (1,)), ((), ())), preferred_element_type=jnp.float32
    )
    shares = lax.psum_scatter(first + second, "dp", scatter_dimension=0, tiled=True)
    returned = lax.all_to_all(
        shares.astype(jnp.bfloat16).reshape(columns, groups, capacity),
        "expert",
        split_axis=1,
        concat_axis=1,
        tiled=True,
    )
    summed = jnp.dot(
        returned.reshape(columns, groups * capacity), picker, preferred_element_type=jnp.float32
    )
    return summed.T.astype(jnp.bfloat16)


def kernel_fits(out_grad, saved_gate):
    columns, hidden = out_grad.shape[1], saved_gate.shape[2]
    return (
        lax.axis_size("dp") == 4
        and lax.axis_size("expert") // SPLIT <= 8
        and columns % TILE == 0
        and hidden % TILE == 0
        and saved_gate.shape[1] % 16 == 0
        and (saved_gate.shape[1] // lax.axis_size("expert")) % 8 == 0
        and 4 * 3 * columns * hidden * 2 <= 40 * 2**20
    )


def either(*args):
    return (local if kernel_fits(args[0], args[3]) else plain_local)(*args)


def solution(mesh):
    in_specs = (
        P("expert", "dp"),
        P("expert", None),
        P("expert", None),
        P("expert", None, "dp"),
        P("expert", None, "dp"),
        P("expert", None, "dp"),
        P("expert", None, "dp"),
        P("expert", "dp", None),
    )
    out_specs = P("expert", "dp")
    return jax.shard_map(either, mesh=mesh, in_specs=in_specs, out_specs=out_specs, check_vma=False)
```

```python
import functools

import jax
import jax.numpy as jnp
from jax import lax
from jax.experimental import pallas as pl
from jax.experimental.pallas import tpu as pltpu
from jax.sharding import PartitionSpec as P

SPLIT = 2
MESH = pl.DeviceIdType.MESH
TILE = 256
NT = (((1,), (1,)), ((), ()))
RETURN_ORDER = (3, 1, 2, 0)


def layer_kernel(
    experts, capacity, columns, hidden,
    ids_ref, ids_t_ref, probs_t_ref, grad_ref, gate_hbm, up_hbm, wg_hbm, wu_hbm, wd_hbm,
    out_ref,
    wd_v, wg_v, wu_v, gate_v, up_v, disp, xbuf, xs, acc, gg, ug,
    pbuf, pair_send, pair_recv, rs_send, rs_recv, back_send, back_recv,
    wd_sem, wg_sem, wu_sem, saved_sem,
    z_ss, z_rs, x_ss, x_rs, f_ss, f_rs, pair_ss, pair_rs, rs_ss, rs_rs, b_ss, b_rs,
):
    groups = experts * SPLIT
    tokens = grad_ref.shape[0]
    d = lax.axis_index("dp")
    g = lax.axis_index("expert")
    z, c = g // SPLIT, g % SPLIT
    sibling = z * SPLIT + (1 - c)
    dx, dy = d % 2, d // 2
    peers = (d, dy * 2 + (1 - dx), (1 - dy) * 2 + dx, (1 - dy) * 2 + (1 - dx))

    def block(r):
        return pl.ds(pl.multiple_of(peers[r] * columns, columns), columns)

    wd_copy = [pltpu.make_async_copy(wd_hbm.at[0, :, block(r)], wd_v.at[r], wd_sem.at[r]) for r in range(4)]
    wg_copy = [pltpu.make_async_copy(wg_hbm.at[0, block(r), :], wg_v.at[r], wg_sem.at[r]) for r in range(4)]
    wu_copy = [pltpu.make_async_copy(wu_hbm.at[0, block(r), :], wu_v.at[r], wu_sem.at[r]) for r in range(4)]
    gate_copy = pltpu.make_async_copy(gate_hbm.at[0], gate_v, saved_sem.at[0])
    up_copy = pltpu.make_async_copy(up_hbm.at[0], up_v, saved_sem.at[1])
    barrier = pltpu.get_barrier_semaphore()
    for k in range(1, experts):
        pl.semaphore_signal(
            barrier, inc=1, device_id=(d, ((z + k) % experts) * SPLIT + c), device_id_type=MESH
        )
    for r in range(1, 4):
        pl.semaphore_signal(barrier, inc=1, device_id=(peers[r], g), device_id_type=MESH)
    pl.semaphore_signal(barrier, inc=1, device_id=(d, sibling), device_id_type=MESH)
    for copy in wd_copy + [gate_copy, up_copy]:
        copy.start()
    for r in RETURN_ORDER:
        wg_copy[r].start()
        wu_copy[r].start()

    row = lax.broadcasted_iota(jnp.int32, (tokens, tokens), 0)
    col = lax.broadcasted_iota(jnp.int32, (tokens, tokens), 1)
    before = (row < col).astype(jnp.bfloat16)
    expert_row = lax.broadcasted_iota(jnp.int32, (8, tokens), 0)
    first, second = ids_t_ref[0:1, :] == expert_row, ids_t_ref[1:2, :] == expert_row
    named = jnp.where(first | second, 1.0, 0.0)
    weight = jnp.where(first, probs_t_ref[0:1, :], 0.0) + jnp.where(second, probs_t_ref[1:2, :], 0.0)
    rank = jnp.dot(named.astype(jnp.bfloat16), before, preferred_element_type=jnp.float32)
    place = lax.broadcasted_iota(jnp.int32, (capacity, tokens), 0).astype(jnp.float32)
    for e in range(experts):
        picked = jnp.where(place == rank[e : e + 1, :], weight[e : e + 1, :], 0.0)
        disp[e] = jnp.dot(
            picked.astype(jnp.bfloat16), grad_ref[...], preferred_element_type=jnp.float32
        ).astype(jnp.bfloat16)

    pl.semaphore_wait(barrier, experts + 3)

    def remote(src, dst, send, recv, device):
        return pltpu.make_async_remote_copy(
            src_ref=src, dst_ref=dst, send_sem=send, recv_sem=recv, device_id=device, device_id_type=MESH
        )

    source = [(z + experts - k) % experts for k in range(experts)]
    target = [(z + k) % experts for k in range(experts)]

    def z_copies(src, dst, send, recv):
        return [None] + [
            remote(src.at[target[k]], dst.at[z], send.at[k], recv.at[k], (d, target[k] * SPLIT + c))
            for k in range(1, experts)
        ]

    out_z = z_copies(disp, xbuf.at[0, c], z_ss, z_rs)
    for copy in out_z[1:]:
        copy.start()
    xbuf[0, c, z] = disp[z]

    def dp_copy(r_from, r_to, k, to):
        return remote(
            xbuf.at[r_from, c, source[k]], xbuf.at[r_to, c, source[k]],
            x_ss.at[r_to, k], x_rs.at[r_to, k], (peers[to], g),
        )

    out_x = [
        None,
        [dp_copy(0, 1, k, 1) for k in range(experts)],
        [dp_copy(0, 2, k, 2) for k in range(experts)],
        [dp_copy(1, 3, k, 2) if k % 2 == 0 else dp_copy(2, 3, k, 1) for k in range(experts)],
    ]
    forward = [
        [
            remote(
                xbuf.at[r, c, source[k]], xbuf.at[r, c, source[k]],
                f_ss.at[r, k], f_rs.at[r, k], (d, sibling),
            )
            for k in range(experts)
        ]
        for r in range(4)
    ]

    def own(k):
        if k > 0:
            out_z[k].wait_recv()
        out_x[1][k].start()
        out_x[2][k].start()
        forward[0][k].start()

    def arrive(r, k):
        out_x[r][k].wait_recv()
        if r == 1 + k % 2:
            out_x[3][k].start()
        forward[r][k].start()

    def load_slots(r):
        xs[...] = jnp.concatenate(
            [xbuf[r, i % SPLIT, i // SPLIT].astype(jnp.float32) for i in range(groups)], axis=0
        ).astype(jnp.bfloat16)

    def project_block(r):
        for k in range(experts):
            forward[r][k].wait_recv()
        load_slots(r)
        wd_copy[r].wait()
        if r == 3:
            gate_copy.wait()
            up_copy.wait()

        def project(n, carry):
            here = pl.ds(pl.multiple_of(n * TILE, TILE), TILE)
            part = lax.dot_general(xs[...], wd_v[r, here, :], NT, preferred_element_type=jnp.float32)
            if r > 0:
                part = acc[:, here] + part
            if r < 3:
                acc[:, here] = part
            else:
                gate = gate_v[:, here].astype(jnp.float32)
                up = up_v[:, here].astype(jnp.float32)
                sig = jax.nn.sigmoid(gate)
                scaled = part * sig
                gg[:, here] = (scaled * up * (1.0 + gate * (1.0 - sig))).astype(jnp.bfloat16)
                ug[:, here] = (scaled * gate).astype(jnp.bfloat16)
            return carry

        lax.fori_loop(0, hidden // TILE, project, 0)

    own(0)
    for k in range(1, experts):
        own(k)
        arrive(1, k - 1)
        arrive(2, k - 1)
    project_block(0)
    arrive(1, experts - 1)
    arrive(2, experts - 1)
    arrive(3, 0)
    project_block(1)
    for k in range(1, experts - 1):
        arrive(3, k)
    project_block(2)
    arrive(3, experts - 1)
    project_block(3)

    pair = [
        remote(pair_send.at[r], pair_recv.at[r], pair_ss.at[r], pair_rs.at[r], (d, sibling)) for r in range(4)
    ]

    def sum_copy(r, k, to):
        return remote(
            rs_send.at[r, target[k]], rs_recv.at[r, target[k]], rs_ss.at[r, k], rs_rs.at[r, k], (peers[to], g)
        )

    out_rs = [None] + [
        [sum_copy(r, k, 1 + k % 2 if r == 3 else r) for k in range(experts)] for r in (1, 2, 3)
    ]
    outward = sorted(range(experts), key=lambda k: -min(k, experts - k))

    def both_halves(r, k):
        return pbuf[r, target[k] * SPLIT + c] + pair_recv[r, target[k]].astype(jnp.float32)

    def pass_on(r, k):
        value = both_halves(r, k)
        if r != 3 and r == 2 - k % 2:
            out_rs[3][k].wait_recv()
            value = value + rs_recv[3, target[k]].astype(jnp.float32)
        rs_send[r, target[k]] = value.astype(jnp.bfloat16)
        out_rs[r][k].start()

    def back_block(r, between):
        wg_copy[r].wait()
        wu_copy[r].wait()

        def back(n, carry):
            here = pl.ds(pl.multiple_of(n * TILE, TILE), TILE)
            part = lax.dot_general(gg[...], wg_v[r, here, :], NT, preferred_element_type=jnp.float32)
            part = part + lax.dot_general(ug[...], wu_v[r, here, :], NT, preferred_element_type=jnp.float32)
            for i in range(groups):
                pbuf[r, i, :, here] = part[i * capacity : (i + 1) * capacity]
            return carry

        tiles = columns // TILE
        lax.fori_loop(0, tiles - 1, back, 0)
        between()
        lax.fori_loop(tiles - 1, tiles, back, 0)
        for s in range(experts):
            pair_send[r, s] = pbuf[r, s * SPLIT + (1 - c)].astype(jnp.bfloat16)
        pair[r].start()

    def pass_diagonal():
        pair[3].wait_recv()
        for k in outward:
            pass_on(3, k)

    def pass_x():
        pair[1].wait_recv()
        for k in outward:
            if k % 2 == 0:
                pass_on(1, k)

    def pass_y():
        pair[2].wait_recv()
        for k in outward:
            if k % 2 == 1:
                pass_on(2, k)
                pass_on(1, k)
        for k in outward:
            if k % 2 == 0:
                pass_on(2, k)

    back_block(3, lambda: None)
    back_block(1, pass_diagonal)
    back_block(2, pass_x)
    back_block(0, pass_y)

    pair[0].wait_recv()
    out_b = z_copies(back_send, back_recv, b_ss, b_rs)
    for k in outward:
        out_rs[1][k].wait_recv()
        out_rs[2][k].wait_recv()
        total = both_halves(0, k)
        for r in (1, 2):
            total = total + rs_recv[r, target[k]].astype(jnp.float32)
        if k > 0:
            back_send[target[k]] = total.astype(jnp.bfloat16)
            out_b[k].start()
        else:
            back_recv[z] = total.astype(jnp.bfloat16)

    after = (col < row).astype(jnp.bfloat16)
    expert_col = lax.broadcasted_iota(jnp.int32, (tokens, 128), 1)
    named_t = (ids_ref[:, 0:1] == expert_col) | (ids_ref[:, 1:2] == expert_col)
    named_t = jnp.where(named_t, 1.0, 0.0)
    rank_t = jnp.dot(after, named_t.astype(jnp.bfloat16), preferred_element_type=jnp.float32)
    place_t = lax.broadcasted_iota(jnp.int32, (tokens, capacity), 1).astype(jnp.float32)
    pickers = [
        jnp.where(place_t == rank_t[:, e : e + 1], named_t[:, e : e + 1], 0.0).astype(jnp.bfloat16)
        for e in range(experts)
    ]
    for copy in out_b[1:]:
        copy.wait_recv()
    result = jnp.dot(pickers[0], back_recv[0], preferred_element_type=jnp.float32)
    for e in range(1, experts):
        result = result + jnp.dot(pickers[e], back_recv[e], preferred_element_type=jnp.float32)
    out_ref[...] = result.astype(jnp.bfloat16)
    for copy in out_z[1:] + sum(out_x[1:] + forward, []) + pair + sum(out_rs[1:], []) + out_b[1:]:
        copy.wait_send()


def local(out_grad, gate_probs, expert_ids, saved_gate, saved_up, w_gate, w_up, w_down):
    groups = lax.axis_size("expert")
    experts = groups // SPLIT
    tokens, columns = out_grad.shape
    slots, hidden = saved_gate.shape[1:]
    capacity = slots // groups
    vmem = pl.BlockSpec(memory_space=pltpu.VMEM)
    hbm = pl.BlockSpec(memory_space=pl.ANY)
    bf16, f32 = jnp.bfloat16, jnp.float32
    dma = pltpu.SemaphoreType.DMA
    return pl.pallas_call(
        functools.partial(layer_kernel, experts, capacity, columns, hidden),
        out_shape=jax.ShapeDtypeStruct((tokens, columns), bf16),
        in_specs=[vmem] * 4 + [hbm] * 5,
        out_specs=vmem,
        scratch_shapes=[
            pltpu.VMEM((4, hidden, columns), bf16),
            pltpu.VMEM((4, columns, hidden), bf16),
            pltpu.VMEM((4, columns, hidden), bf16),
            pltpu.VMEM((slots, hidden), bf16),
            pltpu.VMEM((slots, hidden), bf16),
            pltpu.VMEM((experts, capacity, columns), bf16),
            pltpu.VMEM((4, SPLIT, experts, capacity, columns), bf16),
            pltpu.VMEM((slots, columns), bf16),
            pltpu.VMEM((slots, hidden), f32),
            pltpu.VMEM((slots, hidden), bf16),
            pltpu.VMEM((slots, hidden), bf16),
            pltpu.VMEM((4, groups, capacity, columns), f32),
            pltpu.VMEM((4, experts, capacity, columns), bf16),
            pltpu.VMEM((4, experts, capacity, columns), bf16),
            pltpu.VMEM((4, experts, capacity, columns), bf16),
            pltpu.VMEM((4, experts, capacity, columns), bf16),
            pltpu.VMEM((experts, capacity, columns), bf16),
            pltpu.VMEM((experts, capacity, columns), bf16),
            dma((4,)), dma((4,)), dma((4,)), dma((2,)),
            dma((experts,)), dma((experts,)),
            dma((4, experts)), dma((4, experts)), dma((4, experts)), dma((4, experts)),
            dma((4,)), dma((4,)), dma((4, experts)), dma((4, experts)),
            dma((experts,)), dma((experts,)),
        ],
        compiler_params=pltpu.CompilerParams(
            collective_id=0, has_side_effects=True, vmem_limit_bytes=67043328
        ),
    )(
        expert_ids, expert_ids.T, gate_probs.T.astype(f32), out_grad,
        saved_gate, saved_up, w_gate, w_up, w_down,
    )


def plain_local(out_grad, gate_probs, expert_ids, saved_gate, saved_up, w_gate, w_up, w_down):
    groups = lax.axis_size("expert")
    experts = groups // SPLIT
    columns = out_grad.shape[1]
    tok_rows = out_grad.shape[0]
    slot_count = saved_gate.shape[1]
    capacity = slot_count // groups
    experts_iota = jnp.arange(experts, dtype=jnp.int32)
    chosen = (expert_ids[:, :, None] == experts_iota[None, None, :]).astype(jnp.int32)
    per_token = jnp.sum(chosen, axis=1, dtype=jnp.int32)
    ranked = jnp.cumsum(per_token, axis=0, dtype=jnp.int32) - per_token
    position = jnp.sum(chosen * ranked[:, None, :], axis=2, dtype=jnp.int32)
    target = expert_ids * capacity + position
    slot_iota = jnp.arange(experts * capacity, dtype=jnp.int32)
    matches = slot_iota[:, None, None] == target[None, :, :]
    picker = jnp.any(matches, axis=2).astype(jnp.bfloat16)
    picker = jnp.repeat(picker.reshape(experts, capacity, tok_rows), SPLIT, axis=0).reshape(
        groups * capacity, tok_rows
    )
    weighted = jnp.where(matches, gate_probs.astype(jnp.float32)[None, :, :], 0.0)
    prob_slots = jnp.sum(weighted, axis=(1, 2)).astype(jnp.bfloat16).reshape(experts, capacity)
    prob_slots = jnp.repeat(prob_slots, SPLIT, axis=0)
    down_here = w_down[0]
    dispatched = jnp.dot(picker, out_grad, preferred_element_type=jnp.float32).astype(jnp.bfloat16)
    arrived, arrived_probs = (
        lax.all_to_all(
            dispatched.reshape(groups, capacity, columns),
            "expert",
            split_axis=0,
            concat_axis=0,
            tiled=True,
        ),
        lax.all_to_all(prob_slots, "expert", split_axis=0, concat_axis=0, tiled=True),
    )
    projected = lax.dot_general(
        lax.all_gather(arrived.reshape(slot_count, columns), "dp", axis=1, tiled=True),
        down_here,
        (((1,), (1,)), ((), ())),
        preferred_element_type=jnp.float32,
    )
    gate_pre = saved_gate[0].astype(jnp.float32)
    up_pre = saved_up[0].astype(jnp.float32)
    sigmoid_gate = jax.nn.sigmoid(gate_pre)
    hidden_grad = arrived_probs.reshape(slot_count).astype(jnp.float32)[:, None] * projected
    gate_grad = (
        hidden_grad * up_pre * sigmoid_gate * (1.0 + gate_pre * (1.0 - sigmoid_gate))
    ).astype(jnp.bfloat16)
    up_grad = (hidden_grad * gate_pre * sigmoid_gate).astype(jnp.bfloat16)
    gate_here = w_gate[0]
    up_here = w_up[0]
    first = lax.dot_general(
        gate_here, gate_grad, (((1,), (1,)), ((), ())), preferred_element_type=jnp.float32
    )
    second = lax.dot_general(
        up_here, up_grad, (((1,), (1,)), ((), ())), preferred_element_type=jnp.float32
    )
    shares = lax.psum_scatter(first + second, "dp", scatter_dimension=0, tiled=True)
    returned = lax.all_to_all(
        shares.astype(jnp.bfloat16).reshape(columns, groups, capacity),
        "expert",
        split_axis=1,
        concat_axis=1,
        tiled=True,
    )
    summed = jnp.dot(
        returned.reshape(columns, groups * capacity), picker, preferred_element_type=jnp.float32
    )
    return summed.T.astype(jnp.bfloat16)


def kernel_fits(out_grad, saved_gate):
    columns, hidden = out_grad.shape[1], saved_gate.shape[2]
    return (
        lax.axis_size("dp") == 4
        and lax.axis_size("expert") // SPLIT <= 8
        and columns % TILE == 0
        and hidden % TILE == 0
        and saved_gate.shape[1] % 16 == 0
        and (saved_gate.shape[1] // lax.axis_size("expert")) % 8 == 0
        and 4 * 3 * columns * hidden * 2 <= 40 * 2**20
    )


def either(*args):
    return (local if kernel_fits(args[0], args[3]) else plain_local)(*args)


def solution(mesh):
    in_specs = (
        P("expert", "dp"),
        P("expert", None),
        P("expert", None),
        P("expert", None, "dp"),
        P("expert", None, "dp"),
        P("expert", None, "dp"),
        P("expert", None, "dp"),
        P("expert", "dp", None),
    )
    out_specs = P("expert", "dp")
    return jax.shard_map(either, mesh=mesh, in_specs=in_specs, out_specs=out_specs, check_vma=False)
```

```python
import functools

import jax
import jax.numpy as jnp
from jax import lax
from jax.experimental import pallas as pl
from jax.experimental.pallas import tpu as pltpu
from jax.sharding import PartitionSpec as P

SPLIT = 2
MESH = pl.DeviceIdType.MESH
TILE = 256
NT = (((1,), (1,)), ((), ()))
TN = (((0,), (0,)), ((), ()))
RETURN_ORDER = (3, 1, 2, 0)


def layer_kernel(
    experts, capacity, columns, hidden,
    ids_t_ref, probs_t_ref, grad_ref, gate_hbm, up_hbm, wg_hbm, wu_hbm, wd_hbm,
    out_ref,
    wd_v, wg_v, wu_v, gate_v, up_v, disp, xbuf, xs, acc, gate_factor, up_factor, gg, ug,
    pbuf, pair_send, pair_recv, rs_send, rs_recv, back_send, back_recv,
    wd_sem, wg_sem, wu_sem, saved_sem,
    z_ss, z_rs, x_ss, x_rs, f_ss, f_rs, pair_ss, pair_rs, rs_ss, rs_rs, b_ss, b_rs,
):
    groups = experts * SPLIT
    tokens = grad_ref.shape[0]
    d = lax.axis_index("dp")
    g = lax.axis_index("expert")
    z, c = g // SPLIT, g % SPLIT
    sibling = z * SPLIT + (1 - c)
    dx, dy = d % 2, d // 2
    peers = (d, dy * 2 + (1 - dx), (1 - dy) * 2 + dx, (1 - dy) * 2 + (1 - dx))

    def block(r):
        return pl.ds(pl.multiple_of(peers[r] * columns, columns), columns)

    wd_copy = [pltpu.make_async_copy(wd_hbm.at[0, :, block(r)], wd_v.at[r], wd_sem.at[r]) for r in range(4)]
    wg_copy = [pltpu.make_async_copy(wg_hbm.at[0, block(r), :], wg_v.at[r], wg_sem.at[r]) for r in range(4)]
    wu_copy = [pltpu.make_async_copy(wu_hbm.at[0, block(r), :], wu_v.at[r], wu_sem.at[r]) for r in range(4)]
    gate_copy = pltpu.make_async_copy(gate_hbm.at[0], gate_v, saved_sem.at[0])
    up_copy = pltpu.make_async_copy(up_hbm.at[0], up_v, saved_sem.at[1])
    barrier = pltpu.get_barrier_semaphore()
    for k in range(1, experts):
        pl.semaphore_signal(
            barrier, inc=1, device_id=(d, ((z + k) % experts) * SPLIT + c), device_id_type=MESH
        )
    for r in range(1, 4):
        pl.semaphore_signal(barrier, inc=1, device_id=(peers[r], g), device_id_type=MESH)
    pl.semaphore_signal(barrier, inc=1, device_id=(d, sibling), device_id_type=MESH)
    for copy in [gate_copy, up_copy] + wd_copy:
        copy.start()
    for r in RETURN_ORDER:
        wg_copy[r].start()
        wu_copy[r].start()

    row = lax.broadcasted_iota(jnp.int32, (tokens, tokens), 0)
    col = lax.broadcasted_iota(jnp.int32, (tokens, tokens), 1)
    before = (row < col).astype(jnp.bfloat16)
    expert_row = lax.broadcasted_iota(jnp.int32, (8, tokens), 0)
    first, second = ids_t_ref[0:1, :] == expert_row, ids_t_ref[1:2, :] == expert_row
    named = jnp.where(first | second, 1.0, 0.0)
    probs = probs_t_ref[...].astype(jnp.float32)
    weight = jnp.where(first, probs[0:1, :], 0.0) + jnp.where(second, probs[1:2, :], 0.0)
    rank = jnp.dot(named.astype(jnp.bfloat16), before, preferred_element_type=jnp.float32)
    place = lax.broadcasted_iota(jnp.int32, (capacity, tokens), 0).astype(jnp.float32)
    for e in range(experts):
        picked = jnp.where(place == rank[e : e + 1, :], weight[e : e + 1, :], 0.0)
        disp[e] = jnp.dot(
            picked.astype(jnp.bfloat16), grad_ref[...], preferred_element_type=jnp.float32
        ).astype(jnp.bfloat16)

    pl.semaphore_wait(barrier, experts + 3)

    def remote(src, dst, send, recv, device):
        return pltpu.make_async_remote_copy(
            src_ref=src, dst_ref=dst, send_sem=send, recv_sem=recv, device_id=device, device_id_type=MESH
        )

    source = [(z + experts - k) % experts for k in range(experts)]
    target = [(z + k) % experts for k in range(experts)]

    def z_copies(src, dst, send, recv):
        return [None] + [
            remote(src.at[target[k]], dst.at[z], send.at[k], recv.at[k], (d, target[k] * SPLIT + c))
            for k in range(1, experts)
        ]

    out_z = z_copies(disp, xbuf.at[0, c], z_ss, z_rs)
    for copy in out_z[1:]:
        copy.start()
    xbuf[0, c, z] = disp[z]

    def dp_copy(r_from, r_to, k, to):
        return remote(
            xbuf.at[r_from, c, source[k]], xbuf.at[r_to, c, source[k]],
            x_ss.at[r_to, k], x_rs.at[r_to, k], (peers[to], g),
        )

    out_x = [
        None,
        [dp_copy(0, 1, k, 1) for k in range(experts)],
        [dp_copy(0, 2, k, 2) for k in range(experts)],
        [dp_copy(1, 3, k, 2) if k % 2 == 0 else dp_copy(2, 3, k, 1) for k in range(experts)],
    ]
    forward = [
        [
            remote(
                xbuf.at[r, c, source[k]], xbuf.at[r, c, source[k]],
                f_ss.at[r, k], f_rs.at[r, k], (d, sibling),
            )
            for k in range(experts)
        ]
        for r in range(4)
    ]

    def own(k):
        if k > 0:
            out_z[k].wait_recv()
        out_x[1][k].start()
        out_x[2][k].start()
        forward[0][k].start()

    def arrive(r, k):
        out_x[r][k].wait_recv()
        if r == 1 + k % 2:
            out_x[3][k].start()
        forward[r][k].start()

    def project_blocks(blocks):
        for r in blocks:
            for k in range(experts):
                forward[r][k].wait_recv()
            xs[r % 2] = jnp.concatenate(
                [xbuf[r, i % SPLIT, i // SPLIT].astype(jnp.float32) for i in range(groups)], axis=0
            ).astype(jnp.bfloat16)
            wd_copy[r].wait()

        def project(n, carry):
            here = pl.ds(pl.multiple_of(n * 2 * TILE, 2 * TILE), 2 * TILE)
            part = None
            for r in blocks:
                term = lax.dot_general(xs[r % 2], wd_v[r, here, :], NT, preferred_element_type=jnp.float32)
                part = term if part is None else part + term
            if 0 not in blocks:
                part = acc[:, here] + part
            if 3 not in blocks:
                acc[:, here] = part
            else:
                gg[:, here] = (part * gate_factor[:, here]).astype(jnp.bfloat16)
                ug[:, here] = (part * up_factor[:, here]).astype(jnp.bfloat16)
            return carry

        lax.fori_loop(0, hidden // TILE // 2, project, 0)

    def factors(n, carry):
        here = pl.ds(pl.multiple_of(n * TILE, TILE), TILE)
        gate = gate_v[:, here].astype(jnp.float32)
        up = up_v[:, here].astype(jnp.float32)
        sig = jax.nn.sigmoid(gate)
        gate_factor[:, here] = up * sig * (1.0 + gate * (1.0 - sig))
        up_factor[:, here] = gate * sig
        return carry

    own(0)
    for k in range(1, experts):
        own(k)
        arrive(1, k - 1)
        arrive(2, k - 1)
    gate_copy.wait()
    up_copy.wait()
    lax.fori_loop(0, hidden // TILE, factors, 0)
    project_blocks((0,))
    arrive(1, experts - 1)
    arrive(2, experts - 1)
    for k in range(experts - 1):
        arrive(3, k)
    project_blocks((1, 2))
    arrive(3, experts - 1)
    project_blocks((3,))

    pair = [
        remote(pair_send.at[r], pair_recv.at[r], pair_ss.at[r], pair_rs.at[r], (d, sibling)) for r in range(4)
    ]

    def sum_copy(r, k, to):
        return remote(
            rs_send.at[r, target[k]], rs_recv.at[r, target[k]], rs_ss.at[r, k], rs_rs.at[r, k], (peers[to], g)
        )

    out_rs = [None] + [
        [sum_copy(r, k, 1 + k % 2 if r == 3 else r) for k in range(experts)] for r in (1, 2, 3)
    ]
    outward = sorted(range(experts), key=lambda k: -min(k, experts - k))

    def both_halves(r, k):
        return pbuf[r, target[k] * SPLIT + c] + pair_recv[r, target[k]].astype(jnp.float32)

    def pass_on(r, k):
        value = both_halves(r, k)
        if r != 3 and r == 2 - k % 2:
            out_rs[3][k].wait_recv()
            value = value + rs_recv[3, target[k]].astype(jnp.float32)
        rs_send[r, target[k]] = value.astype(jnp.bfloat16)
        out_rs[r][k].start()

    def back_block(r, between):
        wg_copy[r].wait()
        wu_copy[r].wait()

        def back(n, carry):
            here = pl.ds(pl.multiple_of(n * TILE, TILE), TILE)
            part = lax.dot_general(gg[...], wg_v[r, here, :], NT, preferred_element_type=jnp.float32)
            part = part + lax.dot_general(ug[...], wu_v[r, here, :], NT, preferred_element_type=jnp.float32)
            for i in range(groups):
                pbuf[r, i, :, here] = part[i * capacity : (i + 1) * capacity]
            return carry

        tiles = columns // TILE
        lax.fori_loop(0, tiles - 1, back, 0)
        between()
        lax.fori_loop(tiles - 1, tiles, back, 0)
        for s in range(experts):
            pair_send[r, s] = pbuf[r, s * SPLIT + (1 - c)].astype(jnp.bfloat16)
        pair[r].start()

    def pass_diagonal():
        pair[3].wait_recv()
        for k in outward:
            pass_on(3, k)

    def pass_x():
        pair[1].wait_recv()
        for k in outward:
            if k % 2 == 0:
                pass_on(1, k)

    def pass_y():
        pair[2].wait_recv()
        for k in outward:
            if k % 2 == 1:
                pass_on(2, k)
                pass_on(1, k)
        for k in outward:
            if k % 2 == 0:
                pass_on(2, k)

    back_block(3, lambda: None)
    back_block(1, pass_diagonal)
    back_block(2, pass_x)
    back_block(0, pass_y)

    pair[0].wait_recv()
    out_b = z_copies(back_send, back_recv, b_ss, b_rs)
    for k in outward:
        out_rs[1][k].wait_recv()
        out_rs[2][k].wait_recv()
        total = both_halves(0, k)
        for r in (1, 2):
            total = total + rs_recv[r, target[k]].astype(jnp.float32)
        if k > 0:
            back_send[target[k]] = total.astype(jnp.bfloat16)
            out_b[k].start()
        else:
            back_recv[z] = total.astype(jnp.bfloat16)

    pickers = [
        jnp.where((place == rank[e : e + 1, :]) & (named[e : e + 1, :] > 0.0), 1.0, 0.0).astype(jnp.bfloat16)
        for e in range(experts)
    ]
    for copy in out_b[1:]:
        copy.wait_recv()
    result = lax.dot_general(pickers[0], back_recv[0], TN, preferred_element_type=jnp.float32)
    for e in range(1, experts):
        result = result + lax.dot_general(pickers[e], back_recv[e], TN, preferred_element_type=jnp.float32)
    out_ref[...] = result.astype(jnp.bfloat16)
    for copy in out_z[1:] + sum(out_x[1:] + forward, []) + pair + sum(out_rs[1:], []) + out_b[1:]:
        copy.wait_send()


def local(out_grad, gate_probs, expert_ids, saved_gate, saved_up, w_gate, w_up, w_down):
    groups = lax.axis_size("expert")
    experts = groups // SPLIT
    tokens, columns = out_grad.shape
    slots, hidden = saved_gate.shape[1:]
    capacity = slots // groups
    vmem = pl.BlockSpec(memory_space=pltpu.VMEM)
    hbm = pl.BlockSpec(memory_space=pl.ANY)
    bf16, f32 = jnp.bfloat16, jnp.float32
    dma = pltpu.SemaphoreType.DMA
    return pl.pallas_call(
        functools.partial(layer_kernel, experts, capacity, columns, hidden),
        out_shape=jax.ShapeDtypeStruct((tokens, columns), bf16),
        in_specs=[vmem] * 3 + [hbm] * 5,
        out_specs=vmem,
        scratch_shapes=[
            pltpu.VMEM((4, hidden, columns), bf16),
            pltpu.VMEM((4, columns, hidden), bf16),
            pltpu.VMEM((4, columns, hidden), bf16),
            pltpu.VMEM((slots, hidden), bf16),
            pltpu.VMEM((slots, hidden), bf16),
            pltpu.VMEM((experts, capacity, columns), bf16),
            pltpu.VMEM((4, SPLIT, experts, capacity, columns), bf16),
            pltpu.VMEM((2, slots, columns), bf16),
            pltpu.VMEM((slots, hidden), f32),
            pltpu.VMEM((slots, hidden), f32),
            pltpu.VMEM((slots, hidden), f32),
            pltpu.VMEM((slots, hidden), bf16),
            pltpu.VMEM((slots, hidden), bf16),
            pltpu.VMEM((4, groups, capacity, columns), f32),
            pltpu.VMEM((4, experts, capacity, columns), bf16),
            pltpu.VMEM((4, experts, capacity, columns), bf16),
            pltpu.VMEM((4, experts, capacity, columns), bf16),
            pltpu.VMEM((4, experts, capacity, columns), bf16),
            pltpu.VMEM((experts, capacity, columns), bf16),
            pltpu.VMEM((experts, capacity, columns), bf16),
            dma((4,)), dma((4,)), dma((4,)), dma((2,)),
            dma((experts,)), dma((experts,)),
            dma((4, experts)), dma((4, experts)), dma((4, experts)), dma((4, experts)),
            dma((4,)), dma((4,)), dma((4, experts)), dma((4, experts)),
            dma((experts,)), dma((experts,)),
        ],
        compiler_params=pltpu.CompilerParams(
            collective_id=0, has_side_effects=True, vmem_limit_bytes=67043328
        ),
    )(
        expert_ids.T, gate_probs.T, out_grad,
        saved_gate, saved_up, w_gate, w_up, w_down,
    )


def plain_local(out_grad, gate_probs, expert_ids, saved_gate, saved_up, w_gate, w_up, w_down):
    groups = lax.axis_size("expert")
    experts = groups // SPLIT
    columns = out_grad.shape[1]
    tok_rows = out_grad.shape[0]
    slot_count = saved_gate.shape[1]
    capacity = slot_count // groups
    experts_iota = jnp.arange(experts, dtype=jnp.int32)
    chosen = (expert_ids[:, :, None] == experts_iota[None, None, :]).astype(jnp.int32)
    per_token = jnp.sum(chosen, axis=1, dtype=jnp.int32)
    ranked = jnp.cumsum(per_token, axis=0, dtype=jnp.int32) - per_token
    position = jnp.sum(chosen * ranked[:, None, :], axis=2, dtype=jnp.int32)
    target = expert_ids * capacity + position
    slot_iota = jnp.arange(experts * capacity, dtype=jnp.int32)
    matches = slot_iota[:, None, None] == target[None, :, :]
    picker = jnp.any(matches, axis=2).astype(jnp.bfloat16)
    picker = jnp.repeat(picker.reshape(experts, capacity, tok_rows), SPLIT, axis=0).reshape(
        groups * capacity, tok_rows
    )
    weighted = jnp.where(matches, gate_probs.astype(jnp.float32)[None, :, :], 0.0)
    prob_slots = jnp.sum(weighted, axis=(1, 2)).astype(jnp.bfloat16).reshape(experts, capacity)
    prob_slots = jnp.repeat(prob_slots, SPLIT, axis=0)
    down_here = w_down[0]
    dispatched = jnp.dot(picker, out_grad, preferred_element_type=jnp.float32).astype(jnp.bfloat16)
    arrived, arrived_probs = (
        lax.all_to_all(
            dispatched.reshape(groups, capacity, columns),
            "expert",
            split_axis=0,
            concat_axis=0,
            tiled=True,
        ),
        lax.all_to_all(prob_slots, "expert", split_axis=0, concat_axis=0, tiled=True),
    )
    projected = lax.dot_general(
        lax.all_gather(arrived.reshape(slot_count, columns), "dp", axis=1, tiled=True),
        down_here,
        (((1,), (1,)), ((), ())),
        preferred_element_type=jnp.float32,
    )
    gate_pre = saved_gate[0].astype(jnp.float32)
    up_pre = saved_up[0].astype(jnp.float32)
    sigmoid_gate = jax.nn.sigmoid(gate_pre)
    hidden_grad = arrived_probs.reshape(slot_count).astype(jnp.float32)[:, None] * projected
    gate_grad = (
        hidden_grad * up_pre * sigmoid_gate * (1.0 + gate_pre * (1.0 - sigmoid_gate))
    ).astype(jnp.bfloat16)
    up_grad = (hidden_grad * gate_pre * sigmoid_gate).astype(jnp.bfloat16)
    gate_here = w_gate[0]
    up_here = w_up[0]
    first = lax.dot_general(
        gate_here, gate_grad, (((1,), (1,)), ((), ())), preferred_element_type=jnp.float32
    )
    second = lax.dot_general(
        up_here, up_grad, (((1,), (1,)), ((), ())), preferred_element_type=jnp.float32
    )
    shares = lax.psum_scatter(first + second, "dp", scatter_dimension=0, tiled=True)
    returned = lax.all_to_all(
        shares.astype(jnp.bfloat16).reshape(columns, groups, capacity),
        "expert",
        split_axis=1,
        concat_axis=1,
        tiled=True,
    )
    summed = jnp.dot(
        returned.reshape(columns, groups * capacity), picker, preferred_element_type=jnp.float32
    )
    return summed.T.astype(jnp.bfloat16)


def kernel_fits(out_grad, saved_gate):
    columns, hidden = out_grad.shape[1], saved_gate.shape[2]
    return (
        lax.axis_size("dp") == 4
        and lax.axis_size("expert") // SPLIT <= 8
        and columns % TILE == 0
        and hidden % (2 * TILE) == 0
        and saved_gate.shape[1] % 16 == 0
        and (saved_gate.shape[1] // lax.axis_size("expert")) % 8 == 0
        and 4 * 3 * columns * hidden * 2 <= 40 * 2**20
    )


def either(*args):
    return (local if kernel_fits(args[0], args[3]) else plain_local)(*args)


def solution(mesh):
    in_specs = (
        P("expert", "dp"),
        P("expert", None),
        P("expert", None),
        P("expert", None, "dp"),
        P("expert", None, "dp"),
        P("expert", None, "dp"),
        P("expert", None, "dp"),
        P("expert", "dp", None),
    )
    out_specs = P("expert", "dp")
    return jax.shard_map(either, mesh=mesh, in_specs=in_specs, out_specs=out_specs, check_vma=False)
```
